32 devices in a mesh: row: 16 (over z, x, core), blk: 2 (over y).
Axes of the slice: x: 2, y: 2, z: 4, core: 2. Of those that a mesh axis runs over, the one named last changes fastest.
Arguments:
- embeddings: bfloat16 [8192, 192], P(('row', 'blk')), may hold values from -30 to 30
- vectors: float32 [8192, 16], P(('row', 'blk')), may hold values from -6 to 6
Outputs:
- basis: float32 [8192, 16], P(('row', 'blk'))
- triangle: float32 [16, 16], replicated
The draws below stay inside these ranges and needn't reach their ends.
All inputs are finite; a program needn't handle non-finite values.
Results may differ from the reference program's by a relative error of at most 0.0088.
Values may be sent and summed in bfloat16 or wider, within the bound.
A program may use at most 64 MiB of HBM per device.

```python
import math
import jax
import jax.numpy as jnp
from jax import lax

DIM = 192
VEC = 16
SEGMENTS = 8192


voices = 48


rooms = 4


def draw_embeddings(key, part):
    keys = jax.random.split(jax.random.fold_in(key, 11), 7)
    labels = jax.random.randint(keys[0], (SEGMENTS,), 0, voices)
    places = jax.random.randint(keys[1], (SEGMENTS,), 0, rooms)
    centres = jax.random.normal(keys[2], (voices, DIM), jnp.float32)
    room_dirs = jax.random.normal(keys[3], (rooms, DIM), jnp.float32)
    strength = jax.random.uniform(keys[4], (SEGMENTS, 1), jnp.float32, 0.2, 1.5)
    channel = jax.random.uniform(keys[5], (SEGMENTS, 1), jnp.float32, 0.0, 1.0)
    noise = jax.random.normal(keys[6], (SEGMENTS, DIM), jnp.float32)
    values = 1.5 * strength * centres[labels] + channel * room_dirs[places] + noise
    return jnp.clip(values, -30.0, 30.0).astype(jnp.bfloat16)


def draw_vectors(key, part):
    first, second, third = jax.random.split(jax.random.fold_in(key, 23), 3)
    signs = jnp.where(jax.random.bernoulli(second, 0.5, (VEC,)), 1.0, -1.0)
    offsets = jax.random.uniform(first, (VEC,), jnp.float32, 0.5, 1.0) * signs
    noise = jnp.clip(jax.random.normal(third, (SEGMENTS, VEC), jnp.float32), -4.0, 4.0)
    return jnp.clip(noise + offsets[None, :], -6.0, 6.0)


def setup_inputs(seed: int = 0) -> dict:
    arg_keys = jax.random.split(jax.random.key(seed), 3)
    return {
        "embeddings": draw_embeddings(jax.random.fold_in(arg_keys[2], 71), 0),
        "vectors": draw_vectors(jax.random.fold_in(arg_keys[2], 71), 0),
    }


sharpness = 10.0
epsilon = 1e-06

def normalize(embeddings):
    values = embeddings.astype(jnp.float32)
    return (values * lax.rsqrt(lax.optimization_barrier(jnp.sum(values * values, axis=1, keepdims=True)) + epsilon)).astype(jnp.bfloat16)

def affinity(block_rows, columns):
    scores = lax.dot_general(block_rows.astype(jnp.float32), columns.astype(jnp.float32), (((1,), (1,)), ((), ())), preferred_element_type=jnp.float32)
    return jnp.exp(sharpness * (scores - 1.0))

def reference(embeddings, vectors):
    unit_rows = normalize(embeddings)
    total = unit_rows.shape[0]
    blocks = unit_rows.reshape(-1, math.gcd(total, 512), unit_rows.shape[1])

    def degree_block(block_rows):
        return lax.optimization_barrier(jnp.sum(affinity(block_rows, unit_rows), axis=1))
    degree = lax.map(degree_block, blocks).reshape(total)
    inverse_root = lax.rsqrt(degree)
    weighted = (vectors * inverse_root[:, None]).astype(jnp.bfloat16)

    def apply_block(block_rows):
        tile = affinity(block_rows, unit_rows).astype(jnp.bfloat16)
        return jnp.dot(tile.astype(jnp.float32), weighted.astype(jnp.float32), preferred_element_type=jnp.float32)
    summed = lax.map(apply_block, blocks).reshape(total, vectors.shape[1])
    projected = summed * inverse_root[:, None]
    gram_matrix = jnp.dot(projected.T, projected, precision=lax.Precision.HIGHEST)
    factor = jnp.linalg.cholesky(gram_matrix)
    basis = jax.scipy.linalg.solve_triangular(factor, projected.T, lower=True).T
    return (basis, factor.T)
```

```python
import functools
import math

import jax
import jax.numpy as jnp
from jax import lax
from jax.experimental import pallas as pl
from jax.experimental.pallas import tpu as pltpu
from jax.sharding import PartitionSpec as P

sharpness = 10.0
epsilon = 1e-06
scale2 = sharpness * math.log2(math.e)
MESH = pl.DeviceIdType.MESH
HIGH = lax.Precision.HIGHEST


def flip(bit, by):
    return bit + by - 2 * bit * by


def kernel(plane_line, emb_ref, vec_ref, basis_ref, tri_ref,
           rows, cols, aff, dpart, drecv, wts, spart, srecv, gplane, gline,
           row_s, row_r, col_s, col_r, deg_s, deg_r, wt_s, wt_r, sum_s, sum_r, gp_s, gp_r, gl_s, gl_r):
    blk_low, line = plane_line
    n_local = emb_ref.shape[1]
    r = lax.axis_index("row")
    b = lax.axis_index("blk")
    core, x, y = r % 2, (r // 2) % 2, b % 2
    z = (r // 4) * blk_low + b // 2

    def mate(t):
        c2 = flip(core, t & 1)
        x2 = flip(x, (t >> 1) & 1)
        y2 = flip(y, (t >> 2) & 1)
        return ((r // 4) * 4 + x2 * 2 + c2, (b // 2) * 2 + y2)

    def along(s):
        z2 = (z + s) % line
        return ((z2 // blk_low) * 4 + x * 2 + core, (z2 % blk_low) * 2 + y)

    barrier = pltpu.get_barrier_semaphore()
    for t in range(1, 8):
        pl.semaphore_signal(barrier, inc=1, device_id=mate(t), device_id_type=MESH)
    for s in range(1, line):
        pl.semaphore_signal(barrier, inc=1, device_id=along(s), device_id_type=MESH)

    values = emb_ref[...].astype(jnp.float32)
    norm = lax.rsqrt(jnp.sum(values * values, axis=0, keepdims=True) + epsilon)
    unit = (values * norm).astype(jnp.bfloat16)
    rows[0] = unit
    cols[0] = unit
    pl.semaphore_wait(barrier, 7 + line - 1)

    def send(src, dst, ssem, rsem, to):
        copy = pltpu.make_async_remote_copy(
            src_ref=src, dst_ref=dst, send_sem=ssem, recv_sem=rsem, device_id=to, device_id_type=MESH)
        copy.start()
        return copy

    row_copy = {}
    col_copy = {}
    order = []
    for d in range(1, line // 2 + 1):
        order.append(d)
        if line - d != d:
            order.append(line - d)
    row_copy[1] = send(rows.at[0], rows.at[1], row_s.at[1], row_r.at[1], mate(1))
    for t in (2, 4, 6):
        row_copy[t] = send(rows.at[0], rows.at[t], row_s.at[t], row_r.at[t], mate(t))
    for s in order:
        col_copy[s] = send(cols.at[0], cols.at[s], col_s.at[s], col_r.at[s], along(s))

    def tile(s, t):
        scores = lax.dot_general(cols[s], rows[t], (((0,), (0,)), ((), ())),
                                 preferred_element_type=jnp.float32)
        e = jnp.exp2(scores * scale2 - scale2)
        aff[s, t] = e.astype(jnp.bfloat16)
        part = jnp.sum(e.reshape(n_local // 8, 8, n_local), axis=0)
        return part

    def first(t):
        dpart[t] = tile(0, t)

    first(0)
    for t in (1, 2, 4, 6, 3, 5, 7):
        if t in (2, 4, 6):
            row_copy[t].wait_recv()
            row_copy[t + 1] = send(rows.at[t], rows.at[t + 1], row_s.at[t + 1], row_r.at[t + 1], mate(1))
        else:
            row_copy[t].wait_recv()
        first(t)
    for s in order:
        col_copy[s].wait_recv()

        def body(t, carry):
            dpart[t] = dpart[t] + tile(s, t)
            return carry

        lax.fori_loop(0, 8, body, 0)

    deg_copy = {}
    for t in range(8):
        drecv[8 + t] = jnp.sum(dpart[t], axis=0, keepdims=True)
    for t in range(1, 8):
        deg_copy[t] = send(drecv.at[8 + t], drecv.at[t], deg_s.at[t], deg_r.at[t], mate(t))
    eye = (lax.broadcasted_iota(jnp.int32, (16, 16), 0) == lax.broadcasted_iota(jnp.int32, (16, 16), 1))
    eyef = eye.astype(jnp.float32)
    vec_t = vec_ref[...]
    degree = drecv[8]
    for t in range(1, 8):
        deg_copy[t].wait_recv()
        degree = degree + drecv[t]
    inverse_root = lax.rsqrt(degree)
    wts[0] = (vec_t * inverse_root).astype(jnp.bfloat16)
    wt_copy = {}
    for s in order:
        wt_copy[s] = send(wts.at[0], wts.at[s], wt_s.at[s], wt_r.at[s], along(s))

    def image(s, t):
        return jnp.dot(wts[s], aff[s, t], preferred_element_type=jnp.float32)

    for t in range(8):
        spart[t] = image(0, t)
    for s in order:
        wt_copy[s].wait_recv()
        for t in range(8):
            spart[t] = spart[t] + image(s, t)
    sum_copy = {}
    for t in range(1, 8):
        sum_copy[t] = send(spart.at[t], srecv.at[t], sum_s.at[t], sum_r.at[t], mate(t))
    summed = spart[0]
    for t in range(1, 8):
        sum_copy[t].wait_recv()
        summed = summed + srecv[t]
    projected = summed * inverse_root
    gram = lax.dot_general(projected, projected, (((1,), (1,)), ((), ())), precision=HIGH,
                           preferred_element_type=jnp.float32)
    gplane[0] = gram
    gp_copy = {}
    for t in range(1, 8):
        gp_copy[t] = send(gplane.at[0], gplane.at[t], gp_s.at[t], gp_r.at[t], mate(t))
    for t in range(1, 8):
        gp_copy[t].wait_recv()
    total = ((gram + gplane[1]) + (gplane[2] + gplane[3])) + ((gplane[4] + gplane[5]) + (gplane[6] + gplane[7]))
    gline[0] = total
    gl_copy = {}
    for s in order:
        gl_copy[s] = send(gline.at[0], gline.at[s], gl_s.at[s], gl_r.at[s], along(s))
    for s in order:
        gl_copy[s].wait_recv()
    a = gline[(z + line) % line]
    for k in range(1, line):
        a = a + gline[(z + line - k) % line]

    m = eyef
    below = lax.broadcasted_iota(jnp.int32, (16, 1), 0)
    for k in range(16):
        f = jnp.where(below > k, a[:, k:k + 1] / a[k:k + 1, k:k + 1], 0.0)
        a = a - f * a[k:k + 1, :]
        m = m - f * m[k:k + 1, :]
    root = lax.rsqrt(jnp.sum(jnp.where(eye, a, 0.0), axis=1, keepdims=True))
    upper = lax.broadcasted_iota(jnp.int32, (16, 16), 0) <= lax.broadcasted_iota(jnp.int32, (16, 16), 1)
    tri_ref[...] = jnp.where(upper, a * root, 0.0)
    basis_ref[...] = jnp.dot(m * root, projected, precision=HIGH, preferred_element_type=jnp.float32)

    for group in (row_copy, col_copy, deg_copy, wt_copy, sum_copy, gp_copy, gl_copy):
        for copy in group.values():
            copy.wait_send()


def per_device(sizes, embeddings, vectors):
    blk_low, line = sizes
    n, dim = embeddings.shape
    k = vectors.shape[1]
    dma = pltpu.SemaphoreType.DMA
    vmem = pl.BlockSpec(memory_space=pltpu.VMEM)
    basis_t, tri = pl.pallas_call(
        functools.partial(kernel, sizes),
        out_shape=(jax.ShapeDtypeStruct((k, n), jnp.float32), jax.ShapeDtypeStruct((k, k), jnp.float32)),
        in_specs=[vmem, vmem],
        out_specs=(vmem, vmem),
        scratch_shapes=[
            pltpu.VMEM((8, dim, n), jnp.bfloat16),
            pltpu.VMEM((line, dim, n), jnp.bfloat16),
            pltpu.VMEM((line, 8, n, n), jnp.bfloat16),
            pltpu.VMEM((8, 8, n), jnp.float32),
            pltpu.VMEM((16, 1, n), jnp.float32),
            pltpu.VMEM((line, k, n), jnp.bfloat16),
            pltpu.VMEM((8, k, n), jnp.float32),
            pltpu.VMEM((8, k, n), jnp.float32),
            pltpu.VMEM((8, k, k), jnp.float32),
            pltpu.VMEM((line, k, k), jnp.float32),
            dma((8,)), dma((8,)), dma((line,)), dma((line,)), dma((8,)), dma((8,)),
            dma((line,)), dma((line,)), dma((8,)), dma((8,)), dma((8,)), dma((8,)),
            dma((line,)), dma((line,)),
        ],
        compiler_params=pltpu.CompilerParams(
            collective_id=0, has_side_effects=True, vmem_limit_bytes=60 * 1024 * 1024),
        name="cluster",
    )(embeddings.T, vectors.T)
    return basis_t.T, tri


def solution(mesh):
    blk_low = mesh.shape["blk"] // 2
    line = (mesh.shape["row"] // 4) * blk_low
    placed = (P(("row", "blk"), None), P(("row", "blk"), None))
    return jax.shard_map(
        functools.partial(per_device, (blk_low, line)),
        mesh=mesh,
        in_specs=placed,
        out_specs=(P(("row", "blk"), None), P()),
        check_vma=False,
    )
```

```python
import functools
import math

import jax
import jax.numpy as jnp
from jax import lax
from jax.experimental import pallas as pl
from jax.experimental.pallas import tpu as pltpu
from jax.sharding import PartitionSpec as P

sharpness = 10.0
epsilon = 1e-06
scale2 = sharpness * math.log2(math.e)
MESH = pl.DeviceIdType.MESH
HIGH = lax.Precision.HIGHEST


def flip(bit, by):
    return bit + by - 2 * bit * by


def split(x):
    high = x.astype(jnp.bfloat16)
    rest = x - high.astype(jnp.float32)
    middle = rest.astype(jnp.bfloat16)
    low = (rest - middle.astype(jnp.float32)).astype(jnp.bfloat16)
    return [high, middle, low]


def kernel(plane_line, emb_hbm, vec_hbm, basis_ref, tri_ref, emb_ref, vec_ref, in_sem,
           rows, cols, aff, dpart, drecv, wts, spart, srecv, gplane, gline,
           row_s, row_r, col_s, col_r, deg_s, deg_r, wt_s, wt_r, sum_s, sum_r, gp_s, gp_r, gl_s, gl_r):
    blk_low, line = plane_line
    n_local = emb_ref.shape[1]
    r = lax.axis_index("row")
    b = lax.axis_index("blk")
    core, x, y = r % 2, (r // 2) % 2, b % 2
    z = (r // 4) * blk_low + b // 2

    def mate(t):
        c2 = flip(core, t & 1)
        x2 = flip(x, (t >> 1) & 1)
        y2 = flip(y, (t >> 2) & 1)
        return ((r // 4) * 4 + x2 * 2 + c2, (b // 2) * 2 + y2)

    def toggled(s):
        total, unit_bit = 0, 1
        while unit_bit < line:
            total = total + unit_bit * flip((z // unit_bit) % 2, (s // unit_bit) % 2)
            unit_bit *= 2
        return total

    def along(s):
        z2 = toggled(s)
        return ((z2 // blk_low) * 4 + x * 2 + core, (z2 % blk_low) * 2 + y)

    emb_in = pltpu.make_async_copy(emb_hbm, emb_ref, in_sem.at[0])
    vec_in = pltpu.make_async_copy(vec_hbm, vec_ref, in_sem.at[1])
    emb_in.start()
    vec_in.start()
    barrier = pltpu.get_barrier_semaphore()
    for t in range(1, 8):
        pl.semaphore_signal(barrier, inc=1, device_id=mate(t), device_id_type=MESH)
    for s in range(1, line):
        pl.semaphore_signal(barrier, inc=1, device_id=along(s), device_id_type=MESH)

    emb_in.wait()
    values = emb_ref[...].astype(jnp.float32)
    norm = lax.rsqrt(jnp.sum(values * values, axis=0, keepdims=True) + epsilon)
    unit = (values * norm).astype(jnp.bfloat16)
    rows[0] = unit
    cols[0] = unit
    pl.semaphore_wait(barrier, 7 + line - 1)

    def send(src, dst, ssem, rsem, to):
        copy = pltpu.make_async_remote_copy(
            src_ref=src, dst_ref=dst, send_sem=ssem, recv_sem=rsem, device_id=to, device_id_type=MESH)
        copy.start()
        return copy

    row_copy = {}
    col_copy = {}
    order = list(range(1, line))
    row_copy[1] = send(rows.at[0], rows.at[1], row_s.at[1], row_r.at[1], mate(1))
    for t in (2, 4, 6):
        row_copy[t] = send(rows.at[0], rows.at[t], row_s.at[t], row_r.at[t], mate(t))
    for s in order:
        col_copy[s] = send(cols.at[0], cols.at[s], col_s.at[s], col_r.at[s], along(s))

    def tile(s, t):
        scores = lax.dot_general(cols[s], rows[t], (((0,), (0,)), ((), ())),
                                 preferred_element_type=jnp.float32)
        e = jnp.exp2(scores * scale2 - scale2)
        aff[s, t] = e.astype(jnp.bfloat16)
        part = jnp.sum(e.reshape(n_local // 8, 8, n_local), axis=0)
        return part

    def first(t):
        dpart[t] = tile(0, t)

    first(0)
    for t in (1, 2, 4, 6, 3, 5, 7):
        if t in (2, 4, 6):
            row_copy[t].wait_recv()
            row_copy[t + 1] = send(rows.at[t], rows.at[t + 1], row_s.at[t + 1], row_r.at[t + 1], mate(1))
        else:
            row_copy[t].wait_recv()
        first(t)
    for s in order:
        col_copy[s].wait_recv()

        def body(t, carry):
            dpart[t] = dpart[t] + tile(s, t)
            return carry

        lax.fori_loop(0, 8, body, 0)

    deg_copy = {}
    for t in range(8):
        drecv[8 + t] = jnp.sum(dpart[t], axis=0, keepdims=True)
    for t in range(1, 8):
        deg_copy[t] = send(drecv.at[8 + t], drecv.at[t], deg_s.at[t], deg_r.at[t], mate(t))
    eye = (lax.broadcasted_iota(jnp.int32, (16, 16), 0) == lax.broadcasted_iota(jnp.int32, (16, 16), 1))
    eyef = eye.astype(jnp.float32)
    vec_in.wait()
    vec_t = vec_ref[...]
    degree = drecv[8]
    for t in range(1, 8):
        deg_copy[t].wait_recv()
        degree = degree + drecv[t]
    inverse_root = lax.rsqrt(degree)
    wts[0] = (vec_t * inverse_root).astype(jnp.bfloat16)
    wt_copy = {}
    for s in order:
        wt_copy[s] = send(wts.at[0], wts.at[s], wt_s.at[s], wt_r.at[s], along(s))

    def image(s, t):
        return jnp.dot(wts[s], aff[s, t], preferred_element_type=jnp.float32)

    for t in range(8):
        spart[t] = image(0, t)
    for s in order:
        wt_copy[s].wait_recv()
        for t in range(8):
            spart[t] = spart[t] + image(s, t)
    sum_copy = {}
    for t in range(1, 8):
        sum_copy[t] = send(spart.at[t], srecv.at[t], sum_s.at[t], sum_r.at[t], mate(t))
    summed = spart[0]
    for t in range(1, 8):
        sum_copy[t].wait_recv()
        summed = summed + srecv[t]
    projected = summed * inverse_root
    pieces = jnp.concatenate(split(projected), axis=0)
    products = lax.dot_general(pieces, pieces, (((1,), (1,)), ((), ())),
                               preferred_element_type=jnp.float32)
    halves = products[0:16] + products[16:32] + products[32:48]
    gram = halves[:, 0:16] + halves[:, 16:32] + halves[:, 32:48]
    gplane[0] = gram
    gp_copy = {}
    for t in range(1, 8):
        gp_copy[t] = send(gplane.at[0], gplane.at[t], gp_s.at[t], gp_r.at[t], mate(t))
    for t in range(1, 8):
        gp_copy[t].wait_recv()
    total = ((gram + gplane[1]) + (gplane[2] + gplane[3])) + ((gplane[4] + gplane[5]) + (gplane[6] + gplane[7]))
    gline[0] = total
    gl_copy = {}
    for s in order:
        gl_copy[s] = send(gline.at[0], gline.at[s], gl_s.at[s], gl_r.at[s], along(s))
    for s in order:
        gl_copy[s].wait_recv()
    terms = [gline[s] for s in range(line)]
    while len(terms) > 1:
        terms = [terms[k] + terms[k + 1] for k in range(0, len(terms), 2)]
    a = terms[0]

    m = eyef
    below = lax.broadcasted_iota(jnp.int32, (16, 1), 0)
    for k in range(16):
        f = jnp.where(below > k, a[:, k:k + 1] / a[k:k + 1, k:k + 1], 0.0)
        a = a - f * a[k:k + 1, :]
        m = m - f * m[k:k + 1, :]
    root = lax.rsqrt(jnp.sum(jnp.where(eye, a, 0.0), axis=1, keepdims=True))
    upper = lax.broadcasted_iota(jnp.int32, (16, 16), 0) <= lax.broadcasted_iota(jnp.int32, (16, 16), 1)
    tri_ref[...] = jnp.where(upper, a * root, 0.0)
    basis_ref[...] = jnp.dot(m * root, projected, precision=HIGH, preferred_element_type=jnp.float32)

    for group in (row_copy, col_copy, deg_copy, wt_copy, sum_copy, gp_copy, gl_copy):
        for copy in group.values():
            copy.wait_send()


def per_device(sizes, embeddings, vectors):
    blk_low, line = sizes
    n, dim = embeddings.shape
    k = vectors.shape[1]
    dma = pltpu.SemaphoreType.DMA
    vmem = pl.BlockSpec(memory_space=pltpu.VMEM)
    basis_t, tri = pl.pallas_call(
        functools.partial(kernel, sizes),
        out_shape=(jax.ShapeDtypeStruct((k, n), jnp.float32), jax.ShapeDtypeStruct((k, k), jnp.float32)),
        in_specs=[pl.BlockSpec(memory_space=pl.ANY)] * 2,
        out_specs=(vmem, vmem),
        scratch_shapes=[
            pltpu.VMEM((dim, n), jnp.bfloat16),
            pltpu.VMEM((k, n), jnp.float32),
            dma((2,)),
            pltpu.VMEM((8, dim, n), jnp.bfloat16),
            pltpu.VMEM((line, dim, n), jnp.bfloat16),
            pltpu.VMEM((line, 8, n, n), jnp.bfloat16),
            pltpu.VMEM((8, 8, n), jnp.float32),
            pltpu.VMEM((16, 1, n), jnp.float32),
            pltpu.VMEM((line, k, n), jnp.bfloat16),
            pltpu.VMEM((8, k, n), jnp.float32),
            pltpu.VMEM((8, k, n), jnp.float32),
            pltpu.VMEM((8, k, k), jnp.float32),
            pltpu.VMEM((line, k, k), jnp.float32),
            dma((8,)), dma((8,)), dma((line,)), dma((line,)), dma((8,)), dma((8,)),
            dma((line,)), dma((line,)), dma((8,)), dma((8,)), dma((8,)), dma((8,)),
            dma((line,)), dma((line,)),
        ],
        compiler_params=pltpu.CompilerParams(
            collective_id=0, has_side_effects=True, vmem_limit_bytes=60 * 1024 * 1024),
        name="cluster",
    )(embeddings.T, vectors.T)
    return basis_t.T, tri


def solution(mesh):
    blk_low = mesh.shape["blk"] // 2
    line = (mesh.shape["row"] // 4) * blk_low
    placed = (P(("row", "blk"), None), P(("row", "blk"), None))
    return jax.shard_map(
        functools.partial(per_device, (blk_low, line)),
        mesh=mesh,
        in_specs=placed,
        out_specs=(P(("row", "blk"), None), P()),
        check_vma=False,
    )
```

```python
import functools
import math

import jax
import jax.numpy as jnp
from jax import lax
from jax.experimental import pallas as pl
from jax.experimental.pallas import tpu as pltpu
from jax.sharding import PartitionSpec as P

sharpness = 10.0
epsilon = 1e-06
scale2 = sharpness * math.log2(math.e)
MESH = pl.DeviceIdType.MESH
HIGH = lax.Precision.HIGHEST


def flip(bit, by):
    return bit + by - 2 * bit * by


def split(x):
    high = x.astype(jnp.bfloat16)
    rest = x - high.astype(jnp.float32)
    middle = rest.astype(jnp.bfloat16)
    low = (rest - middle.astype(jnp.float32)).astype(jnp.bfloat16)
    return [high, middle, low]


def kernel(plane_line, emb_hbm, vec_hbm, basis_ref, tri_ref, emb_ref, vec_ref, in_sem,
           rows, cols, turned, aff, dpart, drecv, wts, spart, srecv, gplane, gline,
           row_s, row_r, col_s, col_r, deg_s, deg_r, wt_s, wt_r, sum_s, sum_r, gp_s, gp_r, gl_s, gl_r):
    blk_low, line = plane_line
    n_local = emb_ref.shape[1]
    r = lax.axis_index("row")
    b = lax.axis_index("blk")
    core, x, y = r % 2, (r // 2) % 2, b % 2
    z = (r // 4) * blk_low + b // 2

    def mate(t):
        c2 = flip(core, t & 1)
        x2 = flip(x, (t >> 1) & 1)
        y2 = flip(y, (t >> 2) & 1)
        return ((r // 4) * 4 + x2 * 2 + c2, (b // 2) * 2 + y2)

    def toggled(s):
        total, unit_bit = 0, 1
        while unit_bit < line:
            total = total + unit_bit * flip((z // unit_bit) % 2, (s // unit_bit) % 2)
            unit_bit *= 2
        return total

    def along(s):
        z2 = toggled(s)
        return ((z2 // blk_low) * 4 + x * 2 + core, (z2 % blk_low) * 2 + y)

    emb_in = pltpu.make_async_copy(emb_hbm, emb_ref, in_sem.at[0])
    vec_in = pltpu.make_async_copy(vec_hbm, vec_ref, in_sem.at[1])
    emb_in.start()
    vec_in.start()
    barrier = pltpu.get_barrier_semaphore()
    for t in range(1, 8):
        pl.semaphore_signal(barrier, inc=1, device_id=mate(t), device_id_type=MESH)
    for s in range(1, line):
        pl.semaphore_signal(barrier, inc=1, device_id=along(s), device_id_type=MESH)

    emb_in.wait()
    values = emb_ref[...].astype(jnp.float32)
    norm = lax.rsqrt(jnp.sum(values * values, axis=0, keepdims=True) + epsilon)
    unit = (values * norm).astype(jnp.bfloat16)
    rows[0] = unit
    cols[0] = unit
    pl.semaphore_wait(barrier, 7 + line - 1)

    def send(src, dst, ssem, rsem, to):
        copy = pltpu.make_async_remote_copy(
            src_ref=src, dst_ref=dst, send_sem=ssem, recv_sem=rsem, device_id=to, device_id_type=MESH)
        copy.start()
        return copy

    row_copy = {}
    col_copy = {}
    order = list(range(1, line))
    row_copy[1] = send(rows.at[0], rows.at[1], row_s.at[1], row_r.at[1], mate(1))
    for t in (2, 4, 6):
        row_copy[t] = send(rows.at[0], rows.at[t], row_s.at[t], row_r.at[t], mate(t))
    for s in order:
        col_copy[s] = send(cols.at[0], cols.at[s], col_s.at[s], col_r.at[s], along(s))

    def tile(s, t):
        scores = jnp.dot(turned[s], rows[t], preferred_element_type=jnp.float32)
        e = jnp.exp2(scores * scale2 - scale2)
        aff[s, t] = e.astype(jnp.bfloat16)
        part = jnp.sum(e.reshape(n_local // 8, 8, n_local), axis=0)
        return part

    def turn(s):
        turned[s] = cols[s].astype(jnp.float32).T.astype(jnp.bfloat16)

    turn(0)

    def first(t):
        dpart[t] = tile(0, t)

    first(0)
    for t in (1, 2, 4, 6, 3, 5, 7):
        if t in (2, 4, 6):
            row_copy[t].wait_recv()
            row_copy[t + 1] = send(rows.at[t], rows.at[t + 1], row_s.at[t + 1], row_r.at[t + 1], mate(1))
        else:
            row_copy[t].wait_recv()
        first(t)
    for s in order:
        col_copy[s].wait_recv()
        turn(s)

        def body(t, carry):
            dpart[t] = dpart[t] + tile(s, t)
            return carry

        lax.fori_loop(0, 8, body, 0, unroll=8 if line <= 8 else 1)

    deg_copy = {}
    for t in range(8):
        drecv[8 + t] = jnp.sum(dpart[t], axis=0, keepdims=True)
    for t in range(1, 8):
        deg_copy[t] = send(drecv.at[8 + t], drecv.at[t], deg_s.at[t], deg_r.at[t], mate(t))
    eye = (lax.broadcasted_iota(jnp.int32, (16, 16), 0) == lax.broadcasted_iota(jnp.int32, (16, 16), 1))
    eyef = eye.astype(jnp.float32)
    vec_in.wait()
    vec_t = vec_ref[...]
    degree = drecv[8]
    for t in range(1, 8):
        deg_copy[t].wait_recv()
        degree = degree + drecv[t]
    inverse_root = lax.rsqrt(degree)
    wts[0] = (vec_t * inverse_root).astype(jnp.bfloat16)
    wt_copy = {}
    for s in order:
        wt_copy[s] = send(wts.at[0], wts.at[s], wt_s.at[s], wt_r.at[s], along(s))

    def image(s, t):
        return jnp.dot(wts[s], aff[s, t], preferred_element_type=jnp.float32)

    for t in range(8):
        spart[t] = image(0, t)
    for s in order:
        wt_copy[s].wait_recv()
        for t in range(8):
            spart[t] = spart[t] + image(s, t)
    sum_copy = {}
    for t in range(1, 8):
        sum_copy[t] = send(spart.at[t], srecv.at[t], sum_s.at[t], sum_r.at[t], mate(t))
    summed = spart[0]
    for t in range(1, 8):
        sum_copy[t].wait_recv()
        summed = summed + srecv[t]
    projected = summed * inverse_root
    pieces = jnp.concatenate(split(projected), axis=0)
    products = lax.dot_general(pieces, pieces, (((1,), (1,)), ((), ())),
                               preferred_element_type=jnp.float32)
    halves = products[0:16] + products[16:32] + products[32:48]
    gram = halves[:, 0:16] + halves[:, 16:32] + halves[:, 32:48]
    gram = jnp.concatenate([gram[0:8], gram[8:16]], axis=1)
    gplane[0] = gram
    gp_copy = {}
    for t in range(1, 8):
        gp_copy[t] = send(gplane.at[0], gplane.at[t], gp_s.at[t], gp_r.at[t], mate(t))
    for t in range(1, 8):
        gp_copy[t].wait_recv()
    total = ((gram + gplane[1]) + (gplane[2] + gplane[3])) + ((gplane[4] + gplane[5]) + (gplane[6] + gplane[7]))
    gline[0] = total
    gl_copy = {}
    for s in order:
        gl_copy[s] = send(gline.at[0], gline.at[s], gl_s.at[s], gl_r.at[s], along(s))
    for s in order:
        gl_copy[s].wait_recv()
    terms = [gline[s] for s in range(line)]
    while len(terms) > 1:
        terms = [terms[k] + terms[k + 1] for k in range(0, len(terms), 2)]
    a = jnp.concatenate([terms[0][:, 0:16], terms[0][:, 16:32]], axis=0)

    m = eyef
    below = lax.broadcasted_iota(jnp.int32, (16, 1), 0)
    for k in range(16):
        f = jnp.where(below > k, a[:, k:k + 1] / a[k:k + 1, k:k + 1], 0.0)
        a = a - f * a[k:k + 1, :]
        m = m - f * m[k:k + 1, :]
    root = lax.rsqrt(jnp.sum(jnp.where(eye, a, 0.0), axis=1, keepdims=True))
    upper = lax.broadcasted_iota(jnp.int32, (16, 16), 0) <= lax.broadcasted_iota(jnp.int32, (16, 16), 1)
    tri_ref[...] = jnp.where(upper, a * root, 0.0)
    basis_ref[...] = jnp.dot(m * root, projected, precision=HIGH, preferred_element_type=jnp.float32)

    for group in (row_copy, col_copy, deg_copy, wt_copy, sum_copy, gp_copy, gl_copy):
        for copy in group.values():
            copy.wait_send()


def per_device(sizes, embeddings, vectors):
    blk_low, line = sizes
    n, dim = embeddings.shape
    k = vectors.shape[1]
    dma = pltpu.SemaphoreType.DMA
    vmem = pl.BlockSpec(memory_space=pltpu.VMEM)
    basis_t, tri = pl.pallas_call(
        functools.partial(kernel, sizes),
        out_shape=(jax.ShapeDtypeStruct((k, n), jnp.float32), jax.ShapeDtypeStruct((k, k), jnp.float32)),
        in_specs=[pl.BlockSpec(memory_space=pl.ANY)] * 2,
        out_specs=(vmem, vmem),
        scratch_shapes=[
            pltpu.VMEM((dim, n), jnp.bfloat16),
            pltpu.VMEM((k, n), jnp.float32),
            dma((2,)),
            pltpu.VMEM((8, dim, n), jnp.bfloat16),
            pltpu.VMEM((line, dim, n), jnp.bfloat16),
            pltpu.VMEM((line, n, dim), jnp.bfloat16),
            pltpu.VMEM((line, 8, n, n), jnp.bfloat16),
            pltpu.VMEM((8, 8, n), jnp.float32),
            pltpu.VMEM((16, 1, n), jnp.float32),
            pltpu.VMEM((line, k, n), jnp.bfloat16),
            pltpu.VMEM((8, k, n), jnp.float32),
            pltpu.VMEM((8, k, n), jnp.float32),
            pltpu.VMEM((8, k // 2, 2 * k), jnp.float32),
            pltpu.VMEM((line, k // 2, 2 * k), jnp.float32),
            dma((8,)), dma((8,)), dma((line,)), dma((line,)), dma((8,)), dma((8,)),
            dma((line,)), dma((line,)), dma((8,)), dma((8,)), dma((8,)), dma((8,)),
            dma((line,)), dma((line,)),
        ],
        compiler_params=pltpu.CompilerParams(
            collective_id=0, has_side_effects=True, vmem_limit_bytes=60 * 1024 * 1024),
        name="cluster",
    )(embeddings.T, vectors.T)
    return basis_t.T, tri


def solution(mesh):
    blk_low = mesh.shape["blk"] // 2
    line = (mesh.shape["row"] // 4) * blk_low
    placed = (P(("row", "blk"), None), P(("row", "blk"), None))
    return jax.shard_map(
        functools.partial(per_device, (blk_low, line)),
        mesh=mesh,
        in_specs=placed,
        out_specs=(P(("row", "blk"), None), P()),
        check_vma=False,
    )
```

```python
import functools
import math

import jax
import jax.numpy as jnp
from jax import lax
from jax.experimental import pallas as pl
from jax.experimental.pallas import tpu as pltpu
from jax.sharding import PartitionSpec as P

sharpness = 10.0
epsilon = 1e-06
scale2 = sharpness * math.log2(math.e)
MESH = pl.DeviceIdType.MESH
HIGH = lax.Precision.HIGHEST


def flip(bit, by):
    return bit + by - 2 * bit * by


def split(x):
    high = x.astype(jnp.bfloat16)
    rest = x - high.astype(jnp.float32)
    middle = rest.astype(jnp.bfloat16)
    low = (rest - middle.astype(jnp.float32)).astype(jnp.bfloat16)
    return [high, middle, low]


def kernel(plane_line, emb_hbm, vec_hbm, basis_ref, tri_ref, emb_ref, vec_ref, in_sem,
           rows, cols, turned, aff, dpart, drecv, wts, spart, srecv, gplane, gline,
           row_s, row_r, col_s, col_r, deg_s, deg_r, wt_s, wt_r, sum_s, sum_r, gp_s, gp_r, gl_s, gl_r):
    blk_low, line = plane_line
    n_local = emb_ref.shape[1]
    r = lax.axis_index("row")
    b = lax.axis_index("blk")
    core, x, y = r % 2, (r // 2) % 2, b % 2
    z = (r // 4) * blk_low + b // 2

    def mate(t):
        c2 = flip(core, t & 1)
        x2 = flip(x, (t >> 1) & 1)
        y2 = flip(y, (t >> 2) & 1)
        return ((r // 4) * 4 + x2 * 2 + c2, (b // 2) * 2 + y2)

    def toggled(s):
        total, unit_bit = 0, 1
        while unit_bit < line:
            total = total + unit_bit * flip((z // unit_bit) % 2, (s // unit_bit) % 2)
            unit_bit *= 2
        return total

    def along(s):
        z2 = toggled(s)
        return ((z2 // blk_low) * 4 + x * 2 + core, (z2 % blk_low) * 2 + y)

    emb_in = pltpu.make_async_copy(emb_hbm, emb_ref, in_sem.at[0])
    vec_in = pltpu.make_async_copy(vec_hbm, vec_ref, in_sem.at[1])
    emb_in.start()
    vec_in.start()
    barrier = pltpu.get_barrier_semaphore()
    for t in range(1, 8):
        pl.semaphore_signal(barrier, inc=1, device_id=mate(t), device_id_type=MESH)
    for s in range(1, line):
        pl.semaphore_signal(barrier, inc=1, device_id=along(s), device_id_type=MESH)

    emb_in.wait()
    values = emb_ref[...].astype(jnp.float32)
    norm = lax.rsqrt(jnp.sum(values * values, axis=0, keepdims=True) + epsilon)
    unit = (values * norm).astype(jnp.bfloat16)
    rows[0] = unit
    cols[0] = unit
    pl.semaphore_wait(barrier, 7 + line - 1)

    def send(src, dst, ssem, rsem, to):
        copy = pltpu.make_async_remote_copy(
            src_ref=src, dst_ref=dst, send_sem=ssem, recv_sem=rsem, device_id=to, device_id_type=MESH)
        copy.start()
        return copy

    row_copy = {}
    col_copy = {}
    order = list(range(1, line))
    row_copy[1] = send(rows.at[0], rows.at[1], row_s.at[1], row_r.at[1], mate(1))
    for t in (2, 4, 6):
        row_copy[t] = send(rows.at[0], rows.at[t], row_s.at[t], row_r.at[t], mate(t))
    relayed = line == 4
    half = cols.shape[1] // 2

    def send_part(key, source, slot, start, to):
        part = pl.ds(start, half)
        col_copy[key] = send(cols.at[source, part], cols.at[slot, part], col_s.at[key], col_r.at[key], to)

    if relayed:
        send_part(2, 0, 2, 0, along(2))
        send_part(4, 0, 2, half, along(2))
        col_copy[1] = send(cols.at[0], cols.at[1], col_s.at[1], col_r.at[1], along(1))
        send_part(3, 0, 3, half, along(3))
    else:
        for s in order:
            col_copy[s] = send(cols.at[0], cols.at[s], col_s.at[s], col_r.at[s], along(s))

    def tile(s, t):
        scores = jnp.dot(turned[s], rows[t], preferred_element_type=jnp.float32)
        e = jnp.exp2(scores * scale2 - scale2)
        aff[s, t] = e.astype(jnp.bfloat16)
        part = jnp.sum(e.reshape(n_local // 8, 8, n_local), axis=0)
        return part

    def turn(s):
        turned[s] = cols[s].astype(jnp.float32).T.astype(jnp.bfloat16)

    turn(0)

    def first(t):
        dpart[t] = tile(0, t)

    first(0)
    for t in (1, 2, 4, 6, 3, 5, 7):
        if relayed and t == 6:
            col_copy[2].wait_recv()
            send_part(5, 2, 3, 0, along(1))
        if t in (2, 4, 6):
            row_copy[t].wait_recv()
            row_copy[t + 1] = send(rows.at[t], rows.at[t + 1], row_s.at[t + 1], row_r.at[t + 1], mate(1))
        else:
            row_copy[t].wait_recv()
        first(t)
    for s in order:
        if relayed and s > 1:
            if s == 2:
                col_copy[4].wait_recv()
            else:
                col_copy[3].wait_recv()
                col_copy[5].wait_recv()
        else:
            col_copy[s].wait_recv()
        turn(s)

        def body(t, carry):
            dpart[t] = dpart[t] + tile(s, t)
            return carry

        lax.fori_loop(0, 8, body, 0, unroll=8 if line <= 8 else 1)

    deg_copy = {}
    for t in range(8):
        drecv[8 + t] = jnp.sum(dpart[t], axis=0, keepdims=True)
    for t in range(1, 8):
        deg_copy[t] = send(drecv.at[8 + t], drecv.at[t], deg_s.at[t], deg_r.at[t], mate(t))
    eye = (lax.broadcasted_iota(jnp.int32, (16, 16), 0) == lax.broadcasted_iota(jnp.int32, (16, 16), 1))
    eyef = eye.astype(jnp.float32)
    vec_in.wait()
    vec_t = vec_ref[...]
    degree = drecv[8]
    for t in range(1, 8):
        deg_copy[t].wait_recv()
        degree = degree + drecv[t]
    inverse_root = lax.rsqrt(degree)
    wts[0] = (vec_t * inverse_root).astype(jnp.bfloat16)
    wt_copy = {}
    for s in order:
        wt_copy[s] = send(wts.at[0], wts.at[s], wt_s.at[s], wt_r.at[s], along(s))

    def image(s, t):
        return jnp.dot(wts[s], aff[s, t], preferred_element_type=jnp.float32)

    for t in range(8):
        spart[t] = image(0, t)
    for s in order:
        wt_copy[s].wait_recv()
        for t in range(8):
            spart[t] = spart[t] + image(s, t)
    sum_copy = {}
    for t in range(1, 8):
        sum_copy[t] = send(spart.at[t], srecv.at[t], sum_s.at[t], sum_r.at[t], mate(t))
    summed = spart[0]
    for t in range(1, 8):
        sum_copy[t].wait_recv()
        summed = summed + srecv[t]
    projected = summed * inverse_root
    pieces = jnp.concatenate(split(projected), axis=0)
    products = lax.dot_general(pieces, pieces, (((1,), (1,)), ((), ())),
                               preferred_element_type=jnp.float32)
    halves = products[0:16] + products[16:32] + products[32:48]
    gram = halves[:, 0:16] + halves[:, 16:32] + halves[:, 32:48]
    gram = jnp.concatenate([gram[0:8], gram[8:16]], axis=1)
    gplane[0] = gram
    gp_copy = {}
    for t in range(1, 8):
        gp_copy[t] = send(gplane.at[0], gplane.at[t], gp_s.at[t], gp_r.at[t], mate(t))
    for t in range(1, 8):
        gp_copy[t].wait_recv()
    total = ((gram + gplane[1]) + (gplane[2] + gplane[3])) + ((gplane[4] + gplane[5]) + (gplane[6] + gplane[7]))
    gline[0] = total
    gl_copy = {}
    for s in order:
        gl_copy[s] = send(gline.at[0], gline.at[s], gl_s.at[s], gl_r.at[s], along(s))
    for s in order:
        gl_copy[s].wait_recv()
    terms = [gline[s] for s in range(line)]
    while len(terms) > 1:
        terms = [terms[k] + terms[k + 1] for k in range(0, len(terms), 2)]
    a = jnp.concatenate([terms[0][:, 0:16], terms[0][:, 16:32]], axis=0)

    m = eyef
    below = lax.broadcasted_iota(jnp.int32, (16, 1), 0)
    for k in range(16):
        f = jnp.where(below > k, a[:, k:k + 1] / a[k:k + 1, k:k + 1], 0.0)
        a = a - f * a[k:k + 1, :]
        m = m - f * m[k:k + 1, :]
    root = lax.rsqrt(jnp.sum(jnp.where(eye, a, 0.0), axis=1, keepdims=True))
    upper = lax.broadcasted_iota(jnp.int32, (16, 16), 0) <= lax.broadcasted_iota(jnp.int32, (16, 16), 1)
    tri_ref[...] = jnp.where(upper, a * root, 0.0)
    basis_ref[...] = jnp.dot(m * root, projected, precision=HIGH, preferred_element_type=jnp.float32)

    for group in (row_copy, col_copy, deg_copy, wt_copy, sum_copy, gp_copy, gl_copy):
        for copy in group.values():
            copy.wait_send()


def per_device(sizes, embeddings, vectors):
    blk_low, line = sizes
    n, dim = embeddings.shape
    k = vectors.shape[1]
    dma = pltpu.SemaphoreType.DMA
    vmem = pl.BlockSpec(memory_space=pltpu.VMEM)
    basis_t, tri = pl.pallas_call(
        functools.partial(kernel, sizes),
        out_shape=(jax.ShapeDtypeStruct((k, n), jnp.float32), jax.ShapeDtypeStruct((k, k), jnp.float32)),
        in_specs=[pl.BlockSpec(memory_space=pl.ANY)] * 2,
        out_specs=(vmem, vmem),
        scratch_shapes=[
            pltpu.VMEM((dim, n), jnp.bfloat16),
            pltpu.VMEM((k, n), jnp.float32),
            dma((2,)),
            pltpu.VMEM((8, dim, n), jnp.bfloat16),
            pltpu.VMEM((line, dim, n), jnp.bfloat16),
            pltpu.VMEM((line, n, dim), jnp.bfloat16),
            pltpu.VMEM((line, 8, n, n), jnp.bfloat16),
            pltpu.VMEM((8, 8, n), jnp.float32),
            pltpu.VMEM((16, 1, n), jnp.float32),
            pltpu.VMEM((line, k, n), jnp.bfloat16),
            pltpu.VMEM((8, k, n), jnp.float32),
            pltpu.VMEM((8, k, n), jnp.float32),
            pltpu.VMEM((8, k // 2, 2 * k), jnp.float32),
            pltpu.VMEM((line, k // 2, 2 * k), jnp.float32),
            dma((8,)), dma((8,)), dma((line + 2,)), dma((line + 2,)), dma((8,)), dma((8,)),
            dma((line,)), dma((line,)), dma((8,)), dma((8,)), dma((8,)), dma((8,)),
            dma((line,)), dma((line,)),
        ],
        compiler_params=pltpu.CompilerParams(
            collective_id=0, has_side_effects=True, vmem_limit_bytes=60 * 1024 * 1024),
        name="cluster",
    )(embeddings.T, vectors.T)
    return basis_t.T, tri


def solution(mesh):
    blk_low = mesh.shape["blk"] // 2
    line = (mesh.shape["row"] // 4) * blk_low
    placed = (P(("row", "blk"), None), P(("row", "blk"), None))
    return jax.shard_map(
        functools.partial(per_device, (blk_low, line)),
        mesh=mesh,
        in_specs=placed,
        out_specs=(P(("row", "blk"), None), P()),
        check_vma=False,
    )
```

```python
import functools
import math

import jax
import jax.numpy as jnp
from jax import lax
from jax.experimental import pallas as pl
from jax.experimental.pallas import tpu as pltpu
from jax.sharding import PartitionSpec as P

sharpness = 10.0
epsilon = 1e-06
scale2 = sharpness * math.log2(math.e)
MESH = pl.DeviceIdType.MESH
HIGH = lax.Precision.HIGHEST


def flip(bit, by):
    return bit + by - 2 * bit * by


def split(x):
    high = x.astype(jnp.bfloat16)
    rest = x - high.astype(jnp.float32)
    middle = rest.astype(jnp.bfloat16)
    low = (rest - middle.astype(jnp.float32)).astype(jnp.bfloat16)
    return [high, middle, low]


def kernel(plane_line, emb_hbm, vec_hbm, basis_ref, tri_ref, emb_ref, vec_ref, in_sem,
           rows, cols, turned, aff, dpart, drecv, wts, spart, srecv, gplane, gline,
           row_s, row_r, col_s, col_r, deg_s, deg_r, wt_s, wt_r, sum_s, sum_r, gp_s, gp_r, gl_s, gl_r):
    blk_low, line = plane_line
    n_local = emb_ref.shape[1]
    r = lax.axis_index("row")
    b = lax.axis_index("blk")
    core, x, y = r % 2, (r // 2) % 2, b % 2
    z = (r // 4) * blk_low + b // 2

    def mate(t):
        c2 = flip(core, t & 1)
        x2 = flip(x, (t >> 1) & 1)
        y2 = flip(y, (t >> 2) & 1)
        return ((r // 4) * 4 + x2 * 2 + c2, (b // 2) * 2 + y2)

    def toggled(s):
        total, unit_bit = 0, 1
        while unit_bit < line:
            total = total + unit_bit * flip((z // unit_bit) % 2, (s // unit_bit) % 2)
            unit_bit *= 2
        return total

    def along(s):
        z2 = toggled(s)
        return ((z2 // blk_low) * 4 + x * 2 + core, (z2 % blk_low) * 2 + y)

    emb_in = pltpu.make_async_copy(emb_hbm, emb_ref, in_sem.at[0])
    vec_in = pltpu.make_async_copy(vec_hbm, vec_ref, in_sem.at[1])
    emb_in.start()
    vec_in.start()
    barrier = pltpu.get_barrier_semaphore()
    for t in range(1, 8):
        pl.semaphore_signal(barrier, inc=1, device_id=mate(t), device_id_type=MESH)
    for s in range(1, line):
        pl.semaphore_signal(barrier, inc=1, device_id=along(s), device_id_type=MESH)

    emb_in.wait()
    values = emb_ref[...].astype(jnp.float32)
    norm = lax.rsqrt(jnp.sum(values * values, axis=0, keepdims=True) + epsilon)
    unit = (values * norm).astype(jnp.bfloat16)
    rows[0] = unit
    cols[0] = unit
    pl.semaphore_wait(barrier, 7 + line - 1)

    def send(src, dst, ssem, rsem, to):
        copy = pltpu.make_async_remote_copy(
            src_ref=src, dst_ref=dst, send_sem=ssem, recv_sem=rsem, device_id=to, device_id_type=MESH)
        copy.start()
        return copy

    row_copy = {}
    col_copy = {}
    order = list(range(1, line))
    row_copy[1] = send(rows.at[0], rows.at[1], row_s.at[1], row_r.at[1], mate(1))
    for t in (2, 4, 6):
        row_copy[t] = send(rows.at[0], rows.at[t], row_s.at[t], row_r.at[t], mate(t))
    relayed = line == 4
    half = cols.shape[1] // 2

    def send_part(key, source, slot, start, to):
        part = pl.ds(start, half)
        col_copy[key] = send(cols.at[source, part], cols.at[slot, part], col_s.at[key], col_r.at[key], to)

    if relayed:
        send_part(2, 0, 2, 0, along(2))
        send_part(4, 0, 2, half, along(2))
        col_copy[1] = send(cols.at[0], cols.at[1], col_s.at[1], col_r.at[1], along(1))
        send_part(3, 0, 3, half, along(3))
    else:
        for s in order:
            col_copy[s] = send(cols.at[0], cols.at[s], col_s.at[s], col_r.at[s], along(s))

    def tile(s, t):
        scores = jnp.dot(turned[s], rows[t], preferred_element_type=jnp.float32)
        e = jnp.exp2(scores * scale2 - scale2)
        aff[s, t] = e.astype(jnp.bfloat16)
        part = jnp.sum(e.reshape(n_local // 8, 8, n_local), axis=0)
        return part

    def turn(s):
        turned[s] = cols[s].astype(jnp.float32).T.astype(jnp.bfloat16)

    turn(0)

    def first(t):
        dpart[t] = tile(0, t)

    first(0)
    for t in (1, 2, 4, 6, 3, 5, 7):
        if relayed and t == 6:
            col_copy[2].wait_recv()
            send_part(5, 2, 3, 0, along(1))
        if t in (2, 4, 6):
            row_copy[t].wait_recv()
            row_copy[t + 1] = send(rows.at[t], rows.at[t + 1], row_s.at[t + 1], row_r.at[t + 1], mate(1))
        else:
            row_copy[t].wait_recv()
        first(t)
    for s in order:
        if relayed and s > 1:
            if s == 2:
                col_copy[4].wait_recv()
            else:
                col_copy[3].wait_recv()
                col_copy[5].wait_recv()
        else:
            col_copy[s].wait_recv()
        turn(s)

        def body(t, carry):
            dpart[t] = dpart[t] + tile(s, t)
            return carry

        lax.fori_loop(0, 8, body, 0, unroll=8 if line <= 8 else 1)

    deg_copy = {}
    for t in range(8):
        drecv[8 + t] = jnp.sum(dpart[t], axis=0, keepdims=True)
    for t in range(1, 8):
        deg_copy[t] = send(drecv.at[8 + t], drecv.at[t], deg_s.at[t], deg_r.at[t], mate(t))
    eye = (lax.broadcasted_iota(jnp.int32, (16, 16), 0) == lax.broadcasted_iota(jnp.int32, (16, 16), 1))
    eyef = eye.astype(jnp.float32)
    vec_in.wait()
    vec_t = vec_ref[...]
    degree = drecv[8]
    for t in range(1, 8):
        deg_copy[t].wait_recv()
        degree = degree + drecv[t]
    inverse_root = lax.rsqrt(degree)
    wts[0] = (vec_t * inverse_root).astype(jnp.bfloat16)
    wt_copy = {}
    for s in order:
        wt_copy[s] = send(wts.at[0], wts.at[s], wt_s.at[s], wt_r.at[s], along(s))

    def image(s, t):
        return jnp.dot(wts[s], aff[s, t], preferred_element_type=jnp.float32)

    for t in range(8):
        spart[t] = image(0, t)
    sum_copy = {}
    for s in order:
        wt_copy[s].wait_recv()
        ready = None
        for t in (1, 2, 3, 4, 5, 6, 7, 0):
            spart[t] = spart[t] + image(s, t)
            if s == order[-1]:
                if ready is not None:
                    sum_copy[ready] = send(
                        spart.at[ready], srecv.at[ready], sum_s.at[ready], sum_r.at[ready], mate(ready))
                ready = t
    summed = spart[0]
    for t in range(1, 8):
        sum_copy[t].wait_recv()
        summed = summed + srecv[t]
    projected = summed * inverse_root
    pieces = jnp.concatenate(split(projected), axis=0)
    products = lax.dot_general(pieces, pieces, (((1,), (1,)), ((), ())),
                               preferred_element_type=jnp.float32)
    halves = products[0:16] + products[16:32] + products[32:48]
    gram = halves[:, 0:16] + halves[:, 16:32] + halves[:, 32:48]
    gram = jnp.concatenate([gram[0:8], gram[8:16]], axis=1)
    gplane[0] = gram
    gp_copy = {}
    for t in range(1, 8):
        gp_copy[t] = send(gplane.at[0], gplane.at[t], gp_s.at[t], gp_r.at[t], mate(t))
    for t in range(1, 8):
        gp_copy[t].wait_recv()
    total = ((gram + gplane[1]) + (gplane[2] + gplane[3])) + ((gplane[4] + gplane[5]) + (gplane[6] + gplane[7]))
    gline[0] = total
    gl_copy = {}
    for s in order:
        gl_copy[s] = send(gline.at[0], gline.at[s], gl_s.at[s], gl_r.at[s], along(s))
    for s in order:
        gl_copy[s].wait_recv()
    terms = [gline[s] for s in range(line)]
    while len(terms) > 1:
        terms = [terms[k] + terms[k + 1] for k in range(0, len(terms), 2)]
    a = jnp.concatenate([terms[0][:, 0:16], terms[0][:, 16:32]], axis=0)

    m = eyef
    below = lax.broadcasted_iota(jnp.int32, (16, 1), 0)
    for k in range(16):
        f = jnp.where(below > k, a[:, k:k + 1] / a[k:k + 1, k:k + 1], 0.0)
        a = a - f * a[k:k + 1, :]
        m = m - f * m[k:k + 1, :]
    root = lax.rsqrt(jnp.sum(jnp.where(eye, a, 0.0), axis=1, keepdims=True))
    upper = lax.broadcasted_iota(jnp.int32, (16, 16), 0) <= lax.broadcasted_iota(jnp.int32, (16, 16), 1)
    tri_ref[...] = jnp.where(upper, a * root, 0.0)
    basis_ref[...] = jnp.dot(m * root, projected, precision=HIGH, preferred_element_type=jnp.float32)

    for group in (row_copy, col_copy, deg_copy, wt_copy, sum_copy, gp_copy, gl_copy):
        for copy in group.values():
            copy.wait_send()


def per_device(sizes, embeddings, vectors):
    blk_low, line = sizes
    n, dim = embeddings.shape
    k = vectors.shape[1]
    dma = pltpu.SemaphoreType.DMA
    vmem = pl.BlockSpec(memory_space=pltpu.VMEM)
    basis_t, tri = pl.pallas_call(
        functools.partial(kernel, sizes),
        out_shape=(jax.ShapeDtypeStruct((k, n), jnp.float32), jax.ShapeDtypeStruct((k, k), jnp.float32)),
        in_specs=[pl.BlockSpec(memory_space=pl.ANY)] * 2,
        out_specs=(vmem, vmem),
        scratch_shapes=[
            pltpu.VMEM((dim, n), jnp.bfloat16),
            pltpu.VMEM((k, n), jnp.float32),
            dma((2,)),
            pltpu.VMEM((8, dim, n), jnp.bfloat16),
            pltpu.VMEM((line, dim, n), jnp.bfloat16),
            pltpu.VMEM((line, n, dim), jnp.bfloat16),
            pltpu.VMEM((line, 8, n, n), jnp.bfloat16),
            pltpu.VMEM((8, 8, n), jnp.float32),
            pltpu.VMEM((16, 1, n), jnp.float32),
            pltpu.VMEM((line, k, n), jnp.bfloat16),
            pltpu.VMEM((8, k, n), jnp.float32),
            pltpu.VMEM((8, k, n), jnp.float32),
            pltpu.VMEM((8, k // 2, 2 * k), jnp.float32),
            pltpu.VMEM((line, k // 2, 2 * k), jnp.float32),
            dma((8,)), dma((8,)), dma((line + 2,)), dma((line + 2,)), dma((8,)), dma((8,)),
            dma((line,)), dma((line,)), dma((8,)), dma((8,)), dma((8,)), dma((8,)),
            dma((line,)), dma((line,)),
        ],
        compiler_params=pltpu.CompilerParams(
            collective_id=0, has_side_effects=True, vmem_limit_bytes=60 * 1024 * 1024),
        name="cluster",
    )(embeddings.T, vectors.T)
    return basis_t.T, tri


def solution(mesh):
    blk_low = mesh.shape["blk"] // 2
    line = (mesh.shape["row"] // 4) * blk_low
    placed = (P(("row", "blk"), None), P(("row", "blk"), None))
    return jax.shard_map(
        functools.partial(per_device, (blk_low, line)),
        mesh=mesh,
        in_specs=placed,
        out_specs=(P(("row", "blk"), None), P()),
        check_vma=False,
    )
```
